8 devices in a mesh: fsdp: 4 (over z, y, x), tp: 2 (over core).
Axes of the slice: x: 2, y: 2, z: 1, core: 2. Of those that a mesh axis runs over, the one named last changes fastest.
Arguments:
- x: bfloat16 [32768, 2560], P(('fsdp', 'tp'))
- gamma: float32 [2560], replicated
- w1: bfloat16 [2560, 10240], P('fsdp', 'tp')
- w2: bfloat16 [10240, 2560], P('tp', 'fsdp')
Outputs:
- output: bfloat16 [32768, 2560], P(('fsdp', 'tp'))
All inputs are finite; a program needn't handle non-finite values.
Results may differ from the reference program's by a relative error of at most 0.001.
Values are sent between devices in bfloat16 or wider.
A program may use at most 1 GiB of HBM per device.

```python
import jax
import jax.numpy as jnp
from jax import lax

D = 2560
F = 10240
ROWS = 4096
FSDP = 4
TP = 2

TOK = FSDP * TP * ROWS
BLK = min(ROWS, 512)
EPS = 1e-6


def setup_inputs(seed: int = 0) -> dict:
    k = jax.random.split(jax.random.key(seed), 4)
    x = jax.random.normal(k[0], (TOK, D), jnp.float32).astype(jnp.bfloat16)
    gamma = jax.random.uniform(k[1], (D,), jnp.float32, 0.5, 1.5)
    w1 = (jax.random.normal(k[2], (D, F), jnp.float32) * D ** -0.5).astype(jnp.bfloat16)
    w2 = (jax.random.normal(k[3], (F, D), jnp.float32) * F ** -0.5).astype(jnp.bfloat16)
    return {"x": x, "gamma": gamma, "w1": w1, "w2": w2}


def _block(x, gamma, w1, w2):
    xf = x.astype(jnp.float32)
    mu = jnp.mean(xf, axis=-1, keepdims=True)
    var = jnp.mean(jnp.square(xf - mu), axis=-1, keepdims=True)
    xn = ((xf - mu) * lax.rsqrt(var + EPS) * gamma).astype(jnp.bfloat16)
    h = jax.nn.gelu(jnp.dot(xn, w1, preferred_element_type=jnp.float32), approximate=True).astype(jnp.bfloat16)
    y = jnp.dot(h, w2, preferred_element_type=jnp.float32)
    return (xf + y).astype(jnp.bfloat16)


def reference(x, gamma, w1, w2):
    xb = x.reshape(TOK // BLK, BLK, D)
    yb = lax.map(lambda blk: _block(blk, gamma, w1, w2), xb)
    return yb.reshape(TOK, D)
```

```python
import functools

import jax
import jax.numpy as jnp
from jax import lax
from jax.experimental import pallas as pl
from jax.experimental.pallas import tpu as pltpu
from jax.sharding import PartitionSpec as P

EPS = 1e-6
MESH = pl.DeviceIdType.MESH
BF16 = jnp.bfloat16
F32 = jnp.float32

TOK = 4096
D = 2560
F = 10240
FH = F // 2
DS = D // 4
CH = 256
N1 = FH // CH
NK = 2 * N1
R1 = 1024
S1 = 256
R2 = 512
C2 = 512
K2 = 2 * CH
NS = FH // K2
EXTRA = 6

C0 = 0.7978845608028654
C1 = C0 * 0.044715


def _gelu(x):
    hx = 0.5 * x
    return hx + hx * jnp.tanh(x * (C0 + C1 * (x * x)))


def _kernel(x, gamma, w1, w2, y, h, g1, g2, xs, w2t, sems, wsem, bsem):
    a, b = lax.axis_index("fsdp"), lax.axis_index("tp")
    ax = a + 1 - 2 * lax.rem(a, 2)
    ay = a + 2 - 4 * lax.div(a, 2)
    ad = 3 - a
    chips = (a, ax, ay, ad)
    to_x, to_y, to_c = (ax, b), (ay, b), (a, 1 - b)

    def rows1(k, half):
        cols = pl.ds(pl.multiple_of(k * CH, CH), CH)
        if half is None:
            return (slice(None), cols)
        return (pl.ds(half * (DS // 2), DS // 2), cols)

    def rows2(k, half):
        if half is None:
            return (pl.ds(pl.multiple_of((k - N1) * CH, CH), CH), slice(None))
        hc = CH // 2
        return (pl.ds(pl.multiple_of((k - N1) * CH + half * hc, hc), hc), slice(None))

    class Links:
        def __init__(self, w, g, view):
            self.w, self.g, self.view = w, g, view

        def copy(self, kind, k, src, dst, half, dev):
            v = self.view(k, half)
            s = self.w.at[v] if src is None else self.g.at[(*src, *v)]
            return pltpu.make_async_remote_copy(
                src_ref=s,
                dst_ref=self.g.at[(*dst, *v)],
                send_sem=sems.at[0, kind, k],
                recv_sem=sems.at[1, kind, k],
                device_id=dev,
                device_id_type=MESH,
            )

        def direct(self, k):
            return [
                self.copy(0, k, None, (0, 1), None, to_x),
                self.copy(1, k, None, (0, 2), None, to_y),
            ]

        def forward(self, k):
            return [
                self.copy(2, k, (0, 2), (0, 3), 1, to_x),
                self.copy(3, k, (0, 1), (0, 3), 0, to_y),
            ]

        def core_own(self, k):
            return [self.copy(4, k, None, (1, 0), None, to_c)]

        def core_xy(self, k):
            return [
                self.copy(5, k, (0, 1), (1, 1), None, to_c),
                self.copy(6, k, (0, 2), (1, 2), None, to_c),
            ]

        def core_diag(self, k):
            return [self.copy(7, k, (0, 3), (1, 3), None, to_c)]

    L1, L2 = Links(w1, g1, rows1), Links(w2, g2, rows2)

    def start(copies):
        for c in copies:
            c.start()

    def arrived(copies):
        for c in copies:
            c.wait_recv()

    def ev_direct(ln, k):
        start(ln.direct(k))
        start(ln.core_own(k))

    def ev_forward(ln, k):
        arrived(ln.direct(k))
        start(ln.forward(k))
        start(ln.core_xy(k))

    def ev_diag(ln, k):
        arrived(ln.forward(k))
        start(ln.core_diag(k))

    def ev_here(ln, k):
        arrived(ln.core_own(k) + ln.core_xy(k) + ln.core_diag(k))

    def either(ev, k):
        @pl.when(k < N1)
        def _():
            ev(L1, k)

        @pl.when((k >= N1) & (k < NK))
        def _():
            ev(L2, k)

    def second(ev, k):
        @pl.when(k < NK)
        def _():
            ev(L2, k)

    def half_cols(half, start_col, n):
        off = (b if half == 0 else 1 - b) * FH + start_col
        return pl.ds(pl.multiple_of(off, n), n)

    def load_w2(s):
        slot = lax.rem(s, 2)
        v = (pl.ds(pl.multiple_of(s * K2, K2), K2), slice(None))
        for half in range(2):
            for r in range(4):
                src = w2.at[v] if half == 0 and r == 0 else g2.at[(half, r, *v)]
                cols = pl.ds(pl.multiple_of(chips[r] * DS, 128), DS)
                dst = w2t.at[slot, pl.ds(half * K2, K2), cols]
                pltpu.make_async_copy(src, dst, wsem.at[slot]).start()

    def wait_w2(s):
        slot = lax.rem(s, 2)
        whole = h.at[pl.ds(0, 2 * K2), pl.ds(0, D)]
        pltpu.make_async_copy(whole, w2t.at[slot], wsem.at[slot]).wait()

    def x_block(i):
        return x.at[pl.ds(pl.multiple_of(i * R2, R2), R2), :]

    def x_copy(i):
        slot = lax.rem(i, 2)
        return pltpu.make_async_copy(x_block(i), xs.at[slot], bsem.at[0, slot])

    barrier = pltpu.get_barrier_semaphore()
    for dev in (to_x, to_y, to_c):
        pl.semaphore_signal(barrier, inc=1, device_id=dev, device_id_type=MESH)
    x_copy(0).start()
    pl.semaphore_wait(barrier, 3)
    ev_direct(L1, 0)

    def first(xn, w1t, ht, lsem, osem):
        def load_w1(c):
            slot = lax.rem(c, 2)
            v = rows1(c, None)
            for half in range(2):
                for r in range(4):
                    src = w1.at[v] if half == 0 and r == 0 else g1.at[(half, r, *v)]
                    rows = pl.ds(pl.multiple_of(chips[r] * DS, 128), DS)
                    dst = w1t.at[slot, rows, pl.ds(half * CH, CH)]
                    pltpu.make_async_copy(src, dst, lsem.at[slot]).start()

        def wait_w1(c):
            slot = lax.rem(c, 2)
            whole = h.at[pl.ds(0, D), pl.ds(0, 2 * CH)]
            pltpu.make_async_copy(whole, w1t.at[slot], lsem.at[slot]).wait()

        def norm(i, _):
            slot = lax.rem(i, 2)

            @pl.when(i + 1 < TOK // R2)
            def _():
                x_copy(i + 1).start()

            x_copy(i).wait()

            def group(j, _):
                r = pl.ds(pl.multiple_of(j * 16, 16), 16)
                xf = xs[slot, r, :].astype(F32)
                mu = jnp.mean(xf, axis=-1, keepdims=True)
                d = xf - mu
                var = jnp.mean(d * d, axis=-1, keepdims=True)
                o = pl.ds(pl.multiple_of(i * R2 + j * 16, 16), 16)
                xn[o, :] = (d * lax.rsqrt(var + EPS) * gamma[...]).astype(BF16)
                return 0

            lax.fori_loop(0, R2 // 16, group, 0, unroll=4)

            @pl.when(i == 4)
            def _():
                ev_forward(L1, 0)
                ev_direct(L1, 1)
                ev_direct(L1, 2)

            return 0

        lax.fori_loop(0, TOK // R2, norm, 0)
        ev_diag(L1, 0)
        ev_here(L1, 0)
        load_w1(0)

        def out_copies(i):
            slot = lax.rem(i, 2)
            c, m = lax.div(i, 4), lax.rem(i, 4)
            r = pl.ds(pl.multiple_of(m * R1, R1), R1)
            return [
                pltpu.make_async_copy(
                    ht.at[slot, :, pl.ds(half * CH, CH)],
                    h.at[r, half_cols(half, c * CH, CH)],
                    osem.at[slot],
                )
                for half in range(2)
            ]

        def wait_out(i):
            slot = lax.rem(i, 2)
            whole = h.at[pl.ds(0, R1), pl.ds(0, 2 * CH)]
            pltpu.make_async_copy(ht.at[slot], whole, osem.at[slot]).wait()

        def step(i, _):
            c, m = lax.div(i, 4), lax.rem(i, 4)
            slot = lax.rem(i, 2)
            k = c + 1 + lax.div(c, EXTRA)
            more = lax.rem(c, EXTRA) == EXTRA - 1

            @pl.when(m == 0)
            def _():
                wait_w1(c)
                either(ev_forward, k)
                either(ev_direct, k + 2)

            @pl.when((m == 1) & more)
            def _():
                either(ev_forward, k + 1)
                either(ev_direct, k + 3)

            @pl.when(m == 2)
            def _():
                either(ev_diag, k)

            @pl.when(m == 3)
            def _():
                @pl.when(more)
                def _():
                    either(ev_diag, k + 1)

                @pl.when(c + 1 < N1)
                def _():
                    ev_here(L1, c + 1)
                    load_w1(c + 1)

                @pl.when(c + 1 == N1)
                def _():
                    ev_here(L2, N1)
                    ev_here(L2, N1 + 1)
                    load_w2(0)

            @pl.when(i >= 2)
            def _():
                wait_out(i)

            w = w1t.at[lax.rem(c, 2)]
            for j in range(R1 // S1):
                r = pl.ds(pl.multiple_of(m * R1 + j * S1, S1), S1)
                t = jnp.dot(xn[r, :], w[...], preferred_element_type=F32)
                ht[slot, j * S1 : (j + 1) * S1, :] = _gelu(t).astype(BF16)
            start(out_copies(i))
            return 0

        lax.fori_loop(0, 4 * N1, step, 0)
        wait_out(0)
        wait_out(1)

    pl.run_scoped(
        first,
        pltpu.VMEM((TOK, D), BF16),
        pltpu.VMEM((2, D, 2 * CH), BF16),
        pltpu.VMEM((2, R1, 2 * CH), BF16),
        pltpu.SemaphoreType.DMA((2,)),
        pltpu.SemaphoreType.DMA((2,)),
    )

    k_last = N1 + (N1 - 1) // EXTRA + (1 if N1 % EXTRA == 0 else 0)
    per = TOK // R2

    def rest(acc, ht, hsem):
        def load_h(i):
            slot = lax.rem(i, 2)
            s, m = lax.div(i, per), lax.rem(i, per)
            r = pl.ds(pl.multiple_of(m * R2, R2), R2)
            for half in range(2):
                pltpu.make_async_copy(
                    h.at[r, half_cols(half, s * K2, K2)],
                    ht.at[slot, :, pl.ds(half * K2, K2)],
                    hsem.at[slot],
                ).start()

        def wait_h(i):
            slot = lax.rem(i, 2)
            whole = h.at[pl.ds(0, R2), pl.ds(0, 2 * K2)]
            pltpu.make_async_copy(whole, ht.at[slot], hsem.at[slot]).wait()

        def y_copy(i):
            slot = lax.rem(i, 2)
            m = lax.rem(i, per)
            r = pl.ds(pl.multiple_of(m * R2, R2), R2)
            return pltpu.make_async_copy(xs.at[slot], y.at[r, :], bsem.at[1, slot])

        load_h(0)

        def step(mode, i, _):
            s, m = lax.div(i, per), lax.rem(i, per)
            slot = lax.rem(i, 2)
            k = k_last + 1 + 2 * s

            if mode != "last":
                for q, kk in ((0, k), (4, k + 1)):

                    @pl.when(m == q)
                    def _(kk=kk):
                        second(ev_forward, kk)
                        second(ev_direct, kk + 2)

                    @pl.when(m == q + 2)
                    def _(kk=kk):
                        second(ev_diag, kk)

            @pl.when(m == 0)
            def _():
                wait_w2(s)

            if mode != "last":

                @pl.when(m == per - 1)
                def _():
                    second(ev_here, N1 + 2 * s + 2)
                    second(ev_here, N1 + 2 * s + 3)
                    load_w2(s + 1)

            if mode == "last":

                @pl.when(m == 0)
                def _():
                    x_copy(0).start()

                @pl.when(m >= 1)
                def _():
                    y_copy(i - 1).wait()

                @pl.when(m + 1 < per)
                def _():
                    x_copy(m + 1).start()

            @pl.when(i + 1 < per * NS)
            def _():
                load_h(i + 1)

            wait_h(i)
            r = pl.ds(pl.multiple_of(m * R2, R2), R2)
            w = w2t.at[lax.rem(s, 2)]
            if mode == "last":
                x_copy(m).wait()
            for n in range(D // C2):
                cols = slice(n * C2, (n + 1) * C2)
                t = jnp.dot(ht[slot], w[:, cols], preferred_element_type=F32)
                if mode == "first":
                    acc[r, cols] = t
                elif mode == "mid":
                    acc[r, cols] += t
                else:
                    t = xs[slot, :, cols].astype(F32) + (acc[r, cols] + t)
                    xs[slot, :, cols] = t.astype(BF16)
            if mode == "last":
                y_copy(i).start()
            return 0

        lax.fori_loop(0, per, functools.partial(step, "first"), 0)
        lax.fori_loop(per, per * (NS - 1), functools.partial(step, "mid"), 0)
        lax.fori_loop(per * (NS - 1), per * NS, functools.partial(step, "last"), 0)
        y_copy(per * NS - 1).wait()

    pl.run_scoped(
        rest,
        pltpu.VMEM((TOK, D), F32),
        pltpu.VMEM((2, R2, 2 * K2), BF16),
        pltpu.SemaphoreType.DMA((2,)),
    )

    def drain(ln, k, _):
        for c in ln.direct(k) + ln.forward(k) + ln.core_own(k) + ln.core_xy(k) + ln.core_diag(k):
            c.wait_send()
        return 0

    lax.fori_loop(0, N1, functools.partial(drain, L1), 0)
    lax.fori_loop(N1, NK, functools.partial(drain, L2), 0)


def solution(mesh):
    any_ = pl.BlockSpec(memory_space=pl.ANY)

    def body(x, gamma, w1, w2):
        y, _, _, _ = pl.pallas_call(
            _kernel,
            out_shape=(
                jax.ShapeDtypeStruct((TOK, D), BF16),
                jax.ShapeDtypeStruct((TOK, F), BF16),
                jax.ShapeDtypeStruct((2, 4, DS, FH), BF16),
                jax.ShapeDtypeStruct((2, 4, FH, DS), BF16),
            ),
            in_specs=[any_, pl.BlockSpec(memory_space=pltpu.VMEM), any_, any_],
            out_specs=(any_,) * 4,
            scratch_shapes=[
                pltpu.VMEM((2, R2, D), BF16),
                pltpu.VMEM((2, 2 * K2, D), BF16),
                pltpu.SemaphoreType.DMA((2, 8, NK)),
                pltpu.SemaphoreType.DMA((2,)),
                pltpu.SemaphoreType.DMA((2, 2)),
            ],
            compiler_params=pltpu.CompilerParams(
                collective_id=0, has_side_effects=True, vmem_limit_bytes=67043328
            ),
            name="mlp",
        )(x, gamma.reshape(1, D), w1, w2)
        return y

    return jax.shard_map(
        body,
        mesh=mesh,
        in_specs=(P(("fsdp", "tp"), None), P(None), P("fsdp", "tp"), P("tp", "fsdp")),
        out_specs=P(("fsdp", "tp"), None),
        check_vma=False,
    )
```

```python
import functools

import jax
import jax.numpy as jnp
from jax import lax
from jax.experimental import pallas as pl
from jax.experimental.pallas import tpu as pltpu
from jax.sharding import PartitionSpec as P

EPS = 1e-6
MESH = pl.DeviceIdType.MESH
BF16 = jnp.bfloat16
F32 = jnp.float32

TOK = 4096
D = 2560
F = 10240
FH = F // 2
DS = D // 4
CH = 256
N1 = FH // CH
NK = 2 * N1
R1 = 1024
S1 = 256
R2 = 1024
S2 = 512
RX = 512
RG = 128
C2 = 512
K2 = 2 * CH
NS = FH // K2 - 2
RT = 512
KT = FH - NS * K2
EXTRA = 6

C0 = 0.7978845608028654
C1 = C0 * 0.044715


def _gelu(x):
    hx = 0.5 * x
    return hx + hx * jnp.tanh(x * (C0 + C1 * (x * x)))


def _kernel(x, gamma, w1, w2, acc_out, h, g1, g2, w2t, sems, wsem):
    a, b = lax.axis_index("fsdp"), lax.axis_index("tp")
    ax = a + 1 - 2 * lax.rem(a, 2)
    ay = a + 2 - 4 * lax.div(a, 2)
    ad = 3 - a
    chips = (a, ax, ay, ad)
    to_x, to_y, to_c = (ax, b), (ay, b), (a, 1 - b)

    def rows1(k, half):
        cols = pl.ds(pl.multiple_of(k * CH, CH), CH)
        if half is None:
            return (slice(None), cols)
        return (pl.ds(half * (DS // 2), DS // 2), cols)

    def rows2(k, half):
        if half is None:
            return (pl.ds(pl.multiple_of((k - N1) * CH, CH), CH), slice(None))
        hc = CH // 2
        return (pl.ds(pl.multiple_of((k - N1) * CH + half * hc, hc), hc), slice(None))

    class Links:
        def __init__(self, w, g, view):
            self.w, self.g, self.view = w, g, view

        def copy(self, kind, k, src, dst, half, dev):
            v = self.view(k, half)
            s = self.w.at[v] if src is None else self.g.at[(*src, *v)]
            return pltpu.make_async_remote_copy(
                src_ref=s,
                dst_ref=self.g.at[(*dst, *v)],
                send_sem=sems.at[0, kind, k],
                recv_sem=sems.at[1, kind, k],
                device_id=dev,
                device_id_type=MESH,
            )

        def direct(self, k):
            return [
                self.copy(0, k, None, (0, 1), None, to_x),
                self.copy(1, k, None, (0, 2), None, to_y),
            ]

        def forward(self, k):
            return [
                self.copy(2, k, (0, 2), (0, 3), 1, to_x),
                self.copy(3, k, (0, 1), (0, 3), 0, to_y),
            ]

        def core_own(self, k):
            return [self.copy(4, k, None, (1, 0), None, to_c)]

        def core_xy(self, k):
            return [
                self.copy(5, k, (0, 1), (1, 1), None, to_c),
                self.copy(6, k, (0, 2), (1, 2), None, to_c),
            ]

        def core_diag(self, k):
            return [self.copy(7, k, (0, 3), (1, 3), None, to_c)]

    L1, L2 = Links(w1, g1, rows1), Links(w2, g2, rows2)

    def start(copies):
        for c in copies:
            c.start()

    def arrived(copies):
        for c in copies:
            c.wait_recv()

    def ev_direct(ln, k):
        start(ln.direct(k))
        start(ln.core_own(k))

    def ev_forward(ln, k):
        arrived(ln.direct(k))
        start(ln.forward(k))
        start(ln.core_xy(k))

    def ev_diag(ln, k):
        arrived(ln.forward(k))
        start(ln.core_diag(k))

    def ev_here(ln, k):
        arrived(ln.core_own(k) + ln.core_xy(k) + ln.core_diag(k))

    def either(ev, k):
        @pl.when(k < N1)
        def _():
            ev(L1, k)

        @pl.when((k >= N1) & (k < NK))
        def _():
            ev(L2, k)

    def second(ev, k):
        @pl.when(k < NK)
        def _():
            ev(L2, k)

    def half_cols(half, start_col, n):
        off = (b if half == 0 else 1 - b) * FH + start_col
        return pl.ds(pl.multiple_of(off, n), n)

    def load_w2(s):
        slot = lax.rem(s, 2)
        v = (pl.ds(pl.multiple_of(s * K2, K2), K2), slice(None))
        for half in range(2):
            for r in range(4):
                src = w2.at[v] if half == 0 and r == 0 else g2.at[(half, r, *v)]
                cols = pl.ds(pl.multiple_of(chips[r] * DS, 128), DS)
                dst = w2t.at[slot, pl.ds(half * K2, K2), cols]
                pltpu.make_async_copy(src, dst, wsem.at[slot]).start()

    def wait_w2(s):
        slot = lax.rem(s, 2)
        whole = h.at[pl.ds(0, 2 * K2), pl.ds(0, D)]
        pltpu.make_async_copy(whole, w2t.at[slot], wsem.at[slot]).wait()

    barrier = pltpu.get_barrier_semaphore()
    for dev in (to_x, to_y, to_c):
        pl.semaphore_signal(barrier, inc=1, device_id=dev, device_id_type=MESH)
    pl.semaphore_wait(barrier, 3)
    ev_direct(L1, 0)

    def first(xn, xs, w1t, ht, late, xsem, lsem, osem):
        def x_copy(i):
            slot = lax.rem(i, 2)
            r = pl.ds(pl.multiple_of(i * RX, RX), RX)
            return pltpu.make_async_copy(x.at[r, :], xs.at[slot], xsem.at[slot])

        x_copy(0).start()

        def load_w1(c):
            slot = lax.rem(c, 2)
            v = rows1(c, None)
            for half in range(2):
                for r in range(4):
                    src = w1.at[v] if half == 0 and r == 0 else g1.at[(half, r, *v)]
                    rows = pl.ds(pl.multiple_of(chips[r] * DS, 128), DS)
                    dst = w1t.at[slot, rows, pl.ds(half * CH, CH)]
                    pltpu.make_async_copy(src, dst, lsem.at[slot]).start()

        def wait_w1(c):
            slot = lax.rem(c, 2)
            whole = h.at[pl.ds(0, D), pl.ds(0, 2 * CH)]
            pltpu.make_async_copy(whole, w1t.at[slot], lsem.at[slot]).wait()

        def norm(i, _):
            slot = lax.rem(i, 2)

            @pl.when(i + 1 < TOK // RX)
            def _():
                x_copy(i + 1).start()

            x_copy(i).wait()

            def group(j, _):
                r = pl.ds(pl.multiple_of(j * RG, RG), RG)
                o = pl.ds(pl.multiple_of(i * RX + j * RG, RG), RG)
                tiles = [slice(n * 128, (n + 1) * 128) for n in range(D // 128)]
                t = jnp.zeros((RG, 128), F32)
                for n in tiles:
                    t += xs[slot, r, n].astype(F32)
                mu = jnp.sum(t, axis=-1, keepdims=True) * (1.0 / D)
                t = jnp.zeros((RG, 128), F32)
                for n in tiles:
                    d = xs[slot, r, n].astype(F32) - mu
                    t += d * d
                var = jnp.sum(t, axis=-1, keepdims=True) * (1.0 / D)
                rs = lax.rsqrt(var + EPS)
                for n in tiles:
                    d = xs[slot, r, n].astype(F32) - mu
                    xn[o, n] = (d * rs * gamma[:, n]).astype(BF16)
                return 0

            lax.fori_loop(0, RX // RG, group, 0)

            @pl.when(i == 3)
            def _():
                ev_forward(L1, 0)
                ev_direct(L1, 1)
                ev_direct(L1, 2)

            return 0

        lax.fori_loop(0, TOK // RX, norm, 0)
        ev_diag(L1, 0)
        ev_here(L1, 0)
        load_w1(0)

        def out_copies(i):
            slot = lax.rem(i, 2)
            c, m = lax.div(i, 4), lax.rem(i, 4)
            r = pl.ds(pl.multiple_of(m * R1, R1), R1)
            return [
                pltpu.make_async_copy(
                    ht.at[slot, :, pl.ds(half * CH, CH)],
                    h.at[r, half_cols(half, c * CH, CH)],
                    osem.at[slot],
                )
                for half in range(2)
            ]

        def wait_out(i):
            slot = lax.rem(i, 2)
            whole = h.at[pl.ds(0, R1), pl.ds(0, 2 * CH)]
            pltpu.make_async_copy(ht.at[slot], whole, osem.at[slot]).wait()

        late[...] = jnp.zeros_like(late)
        top = R1 - S1

        def step(i, _):
            c, m = lax.div(i, 4), lax.rem(i, 4)
            slot = lax.rem(i, 2)
            lead = lax.div(c, EXTRA)
            more = lax.rem(c, EXTRA) == EXTRA - 1
            k = c + 1 + lead
            g = c + 1 + jnp.maximum(lead - 1, 0)

            @pl.when(m == 0)
            def _():
                wait_w1(c)
                either(ev_forward, k)

                @pl.when(c <= EXTRA)
                def _():
                    either(ev_direct, k + 2)

                @pl.when(c >= EXTRA)
                def _():
                    either(ev_direct, k + 3)

            @pl.when((m == 1) & more)
            def _():
                either(ev_forward, k + 1)

                @pl.when(c < EXTRA)
                def _():
                    either(ev_direct, k + 3)

                @pl.when(c > EXTRA)
                def _():
                    either(ev_direct, k + 4)

            @pl.when(m == 2)
            def _():
                either(ev_diag, g)

            @pl.when(m == 3)
            def _():
                @pl.when(more & (c > EXTRA))
                def _():
                    either(ev_diag, g + 1)

                @pl.when(c + 1 < N1)
                def _():
                    ev_here(L1, c + 1)
                    load_w1(c + 1)

                @pl.when(c + 1 == N1)
                def _():
                    ev_here(L2, N1)
                    ev_here(L2, N1 + 1)
                    load_w2(0)

            @pl.when(i >= 2)
            def _():
                wait_out(i)

            w = w1t.at[lax.rem(c, 2)]
            before = late[...]
            for j in range(R1 // S1):
                r = pl.ds(pl.multiple_of(m * R1 + j * S1, S1), S1)
                t = jnp.dot(xn[r, :], w[...], preferred_element_type=F32)
                if j == 0:
                    ht[1 - slot, top:, :] = _gelu(before).astype(BF16)
                if j < R1 // S1 - 1:
                    ht[slot, j * S1 : (j + 1) * S1, :] = _gelu(t).astype(BF16)
                else:
                    late[...] = t

            @pl.when(i >= 1)
            def _():
                start(out_copies(i - 1))

            return 0

        n = 4 * N1
        lax.fori_loop(0, n, step, 0)
        wait_out(0)
        ht[(n - 1) % 2, top:, :] = _gelu(late[...]).astype(BF16)
        start(out_copies(n - 1))
        wait_out(1)

    pl.run_scoped(
        first,
        pltpu.VMEM((TOK, D), BF16),
        pltpu.VMEM((2, RX, D), BF16),
        pltpu.VMEM((2, D, 2 * CH), BF16),
        pltpu.VMEM((2, R1, 2 * CH), BF16),
        pltpu.VMEM((S1, 2 * CH), F32),
        pltpu.SemaphoreType.DMA((2,)),
        pltpu.SemaphoreType.DMA((2,)),
        pltpu.SemaphoreType.DMA((2,)),
    )

    k_last = N1 + (N1 - 1) // EXTRA + (1 if N1 % EXTRA == 0 else 0)
    per = TOK // R2

    def rest(acc, ht, hsem, asem):
        def load_h(i):
            slot = lax.rem(i, 2)
            s, m = lax.div(i, per), lax.rem(i, per)
            r = pl.ds(pl.multiple_of(m * R2, R2), R2)
            for half in range(2):
                pltpu.make_async_copy(
                    h.at[r, half_cols(half, s * K2, K2)],
                    ht.at[slot, :, pl.ds(half * K2, K2)],
                    hsem.at[slot],
                ).start()

        def wait_h(i):
            slot = lax.rem(i, 2)
            whole = h.at[pl.ds(0, R2), pl.ds(0, 2 * K2)]
            pltpu.make_async_copy(whole, ht.at[slot], hsem.at[slot]).wait()

        def acc_copy(m):
            r = pl.ds(pl.multiple_of(m * R2, R2), R2)
            return pltpu.make_async_copy(acc.at[r, :], acc_out.at[r, :], asem.at[m])

        load_h(0)

        def step(first_slot, i, _):
            s, m = lax.div(i, per), lax.rem(i, per)
            slot = lax.rem(i, 2)
            k = k_last + 1 + 2 * s

            for q in range(2):

                @pl.when(m == 2 * q)
                def _(q=q):
                    second(ev_forward, k + q)
                    second(ev_direct, k + q + 3)

                @pl.when(m == 2 * q + 1)
                def _(q=q):
                    second(ev_diag, k - 1 + q)

            @pl.when(m == 0)
            def _():
                wait_w2(s)

            @pl.when((m == per - 1) & (s + 1 < NS))
            def _():
                ev_here(L2, N1 + 2 * s + 2)
                ev_here(L2, N1 + 2 * s + 3)
                load_w2(s + 1)

            @pl.when(i + 1 < per * NS)
            def _():
                load_h(i + 1)

            wait_h(i)
            w = w2t.at[lax.rem(s, 2)]
            for j in range(R2 // S2):
                r = pl.ds(pl.multiple_of(m * R2 + j * S2, S2), S2)
                for n in range(D // C2):
                    cols = slice(n * C2, (n + 1) * C2)
                    hj = ht[slot, j * S2 : (j + 1) * S2, :]
                    t = jnp.dot(hj, w[:, cols], preferred_element_type=F32)
                    if first_slot:
                        acc[r, cols] = t
                    else:
                        acc[r, cols] += t

            @pl.when(s == NS - 1)
            def _():
                acc_copy(m).start()

            return 0

        lax.fori_loop(0, per, functools.partial(step, True), 0)
        lax.fori_loop(per, per * NS, functools.partial(step, False), 0)
        for m in range(per):
            acc_copy(m).wait()

    pl.run_scoped(
        rest,
        pltpu.VMEM((TOK, D), F32),
        pltpu.VMEM((2, R2, 2 * K2), BF16),
        pltpu.SemaphoreType.DMA((2,)),
        pltpu.SemaphoreType.DMA((per,)),
    )

    ev_diag(L2, NK - 1)

    def last(k, _):
        ev_here(L2, k)
        return 0

    lax.fori_loop(N1 + 2 * NS, NK, last, 0)

    def drain(ln, k, _):
        for c in ln.direct(k) + ln.forward(k) + ln.core_own(k) + ln.core_xy(k) + ln.core_diag(k):
            c.wait_send()
        return 0

    lax.fori_loop(0, N1, functools.partial(drain, L1), 0)
    lax.fori_loop(N1, NK, functools.partial(drain, L2), 0)


def _tail(x, acc, h0, h1, w2, g2, y, wt, sem):
    @pl.when(pl.program_id(0) == 0)
    def _():
        a, b = lax.axis_index("fsdp"), lax.axis_index("tp")
        ax = a + 1 - 2 * lax.rem(a, 2)
        ay = a + 2 - 4 * lax.div(a, 2)
        chips = (a, ax, ay, 3 - a)
        for half in range(2):
            for r in range(4):
                v = (pl.ds(FH - KT, KT), slice(None))
                src = w2.at[v] if half == 0 and r == 0 else g2.at[(half, r, *v)]
                rows = pl.ds(pl.multiple_of((b if half == 0 else 1 - b) * KT, KT), KT)
                cols = pl.ds(pl.multiple_of(chips[r] * DS, 128), DS)
                pltpu.make_async_copy(src, wt.at[rows, cols], sem).start()
        pltpu.make_async_copy(wt, wt, sem).wait()

    for n in range(D // C2):
        cols = slice(n * C2, (n + 1) * C2)
        t = jnp.dot(h0[...], wt[:KT, cols], preferred_element_type=F32)
        t += jnp.dot(h1[...], wt[KT:, cols], preferred_element_type=F32)
        y[:, cols] = (x[:, cols].astype(F32) + (acc[:, cols] + t)).astype(BF16)


def solution(mesh):
    any_ = pl.BlockSpec(memory_space=pl.ANY)

    def body(x, gamma, w1, w2):
        acc, h, _, g2 = pl.pallas_call(
            _kernel,
            out_shape=(
                jax.ShapeDtypeStruct((TOK, D), F32),
                jax.ShapeDtypeStruct((TOK, F), BF16),
                jax.ShapeDtypeStruct((2, 4, DS, FH), BF16),
                jax.ShapeDtypeStruct((2, 4, FH, DS), BF16),
            ),
            in_specs=[any_, pl.BlockSpec(memory_space=pltpu.VMEM), any_, any_],
            out_specs=(any_,) * 4,
            scratch_shapes=[
                pltpu.VMEM((2, 2 * K2, D), BF16),
                pltpu.SemaphoreType.DMA((2, 8, NK)),
                pltpu.SemaphoreType.DMA((2,)),
            ],
            compiler_params=pltpu.CompilerParams(
                collective_id=0, has_side_effects=True, vmem_limit_bytes=67043328
            ),
            name="mlp",
        )(x, gamma.reshape(1, D), w1, w2)
        return pl.pallas_call(
            _tail,
            grid=(TOK // RT,),
            out_shape=jax.ShapeDtypeStruct((TOK, D), BF16),
            in_specs=[
                pl.BlockSpec((RT, D), lambda m: (m, 0)),
                pl.BlockSpec((RT, D), lambda m: (m, 0)),
                pl.BlockSpec((RT, KT), lambda m: (m, FH // KT - 1)),
                pl.BlockSpec((RT, KT), lambda m: (m, F // KT - 1)),
                any_,
                any_,
            ],
            out_specs=pl.BlockSpec((RT, D), lambda m: (m, 0)),
            scratch_shapes=[pltpu.VMEM((2 * KT, D), BF16), pltpu.SemaphoreType.DMA],
            compiler_params=pltpu.CompilerParams(vmem_limit_bytes=60 * 2**20),
            name="tail",
        )(x, acc, h, h, w2, g2)

    return jax.shard_map(
        body,
        mesh=mesh,
        in_specs=(P(("fsdp", "tp"), None), P(None), P("fsdp", "tp"), P("tp", "fsdp")),
        out_specs=P(("fsdp", "tp"), None),
        check_vma=False,
    )
```

```python
import functools

import jax
import jax.numpy as jnp
from jax import lax
from jax.experimental import pallas as pl
from jax.experimental.pallas import tpu as pltpu
from jax.sharding import PartitionSpec as P

EPS = 1e-6
MESH = pl.DeviceIdType.MESH
BF16 = jnp.bfloat16
F32 = jnp.float32

TOK = 4096
D = 2560
F = 10240
FH = F // 2
DS = D // 4
CH = 256
N1 = FH // CH
NK = 2 * N1
R1 = 2048
S1 = 256
R2 = 1024
S2 = 512
RX = 512
RG = 128
C2 = 512
K2 = 2 * CH
NS = FH // K2 - 2
RT = 512
KT = FH - NS * K2
EXTRA = 6

C0 = 0.7978845608028654
C1 = C0 * 0.044715


def _gelu(x):
    hx = 0.5 * x
    return hx + hx * jnp.tanh(x * (C0 + C1 * (x * x)))


def _kernel(x, gamma, w1, w2, acc_out, h, g1, g2, w2t, sems, wsem):
    a, b = lax.axis_index("fsdp"), lax.axis_index("tp")
    ax = a + 1 - 2 * lax.rem(a, 2)
    ay = a + 2 - 4 * lax.div(a, 2)
    ad = 3 - a
    chips = (a, ax, ay, ad)
    to_x, to_y, to_c = (ax, b), (ay, b), (a, 1 - b)

    def rows1(k, half):
        cols = pl.ds(pl.multiple_of(k * CH, CH), CH)
        if half is None:
            return (slice(None), cols)
        return (pl.ds(half * (DS // 2), DS // 2), cols)

    def rows2(k, half):
        if half is None:
            return (pl.ds(pl.multiple_of((k - N1) * CH, CH), CH), slice(None))
        hc = CH // 2
        return (pl.ds(pl.multiple_of((k - N1) * CH + half * hc, hc), hc), slice(None))

    class Links:
        def __init__(self, w, g, view):
            self.w, self.g, self.view = w, g, view

        def copy(self, kind, k, src, dst, half, dev):
            v = self.view(k, half)
            s = self.w.at[v] if src is None else self.g.at[(*src, *v)]
            return pltpu.make_async_remote_copy(
                src_ref=s,
                dst_ref=self.g.at[(*dst, *v)],
                send_sem=sems.at[0, kind, k],
                recv_sem=sems.at[1, kind, k],
                device_id=dev,
                device_id_type=MESH,
            )

        def direct(self, k):
            return [
                self.copy(0, k, None, (0, 1), None, to_x),
                self.copy(1, k, None, (0, 2), None, to_y),
            ]

        def forward(self, k):
            return [
                self.copy(2, k, (0, 2), (0, 3), 1, to_x),
                self.copy(3, k, (0, 1), (0, 3), 0, to_y),
            ]

        def core_own(self, k):
            return [self.copy(4, k, None, (1, 0), None, to_c)]

        def core_xy(self, k):
            return [
                self.copy(5, k, (0, 1), (1, 1), None, to_c),
                self.copy(6, k, (0, 2), (1, 2), None, to_c),
            ]

        def core_diag(self, k):
            return [self.copy(7, k, (0, 3), (1, 3), None, to_c)]

    L1, L2 = Links(w1, g1, rows1), Links(w2, g2, rows2)

    def start(copies):
        for c in copies:
            c.start()

    def arrived(copies):
        for c in copies:
            c.wait_recv()

    def ev_direct(ln, k):
        start(ln.direct(k))
        start(ln.core_own(k))

    def ev_forward(ln, k):
        arrived(ln.direct(k))
        start(ln.forward(k))
        start(ln.core_xy(k))

    def ev_diag(ln, k):
        arrived(ln.forward(k))
        start(ln.core_diag(k))

    def ev_here(ln, k):
        arrived(ln.core_own(k) + ln.core_xy(k) + ln.core_diag(k))

    def either(ev, k):
        @pl.when(k < N1)
        def _():
            ev(L1, k)

        @pl.when((k >= N1) & (k < NK))
        def _():
            ev(L2, k)

    def second(ev, k):
        @pl.when(k < NK)
        def _():
            ev(L2, k)

    def half_cols(half, start_col, n):
        off = (b if half == 0 else 1 - b) * FH + start_col
        return pl.ds(pl.multiple_of(off, n), n)

    def load_w2(s):
        slot = lax.rem(s, 2)
        v = (pl.ds(pl.multiple_of(s * K2, K2), K2), slice(None))
        for half in range(2):
            for r in range(4):
                src = w2.at[v] if half == 0 and r == 0 else g2.at[(half, r, *v)]
                cols = pl.ds(pl.multiple_of(chips[r] * DS, 128), DS)
                dst = w2t.at[slot, pl.ds(half * K2, K2), cols]
                pltpu.make_async_copy(src, dst, wsem.at[slot]).start()

    def wait_w2(s):
        slot = lax.rem(s, 2)
        whole = h.at[pl.ds(0, 2 * K2), pl.ds(0, D)]
        pltpu.make_async_copy(whole, w2t.at[slot], wsem.at[slot]).wait()

    barrier = pltpu.get_barrier_semaphore()
    for dev in (to_x, to_y, to_c):
        pl.semaphore_signal(barrier, inc=1, device_id=dev, device_id_type=MESH)
    pl.semaphore_wait(barrier, 3)
    ev_direct(L1, 0)

    def first(xn, xs, w1t, ht, xsem, lsem, osem):
        def x_copy(i):
            slot = lax.rem(i, 2)
            r = pl.ds(pl.multiple_of(i * RX, RX), RX)
            return pltpu.make_async_copy(x.at[r, :], xs.at[slot], xsem.at[slot])

        x_copy(0).start()

        def load_w1(c):
            slot = lax.rem(c, 2)
            v = rows1(c, None)
            for half in range(2):
                for r in range(4):
                    src = w1.at[v] if half == 0 and r == 0 else g1.at[(half, r, *v)]
                    rows = pl.ds(pl.multiple_of(chips[r] * DS, 128), DS)
                    dst = w1t.at[slot, rows, pl.ds(half * CH, CH)]
                    pltpu.make_async_copy(src, dst, lsem.at[slot]).start()

        def wait_w1(c):
            slot = lax.rem(c, 2)
            whole = h.at[pl.ds(0, D), pl.ds(0, 2 * CH)]
            pltpu.make_async_copy(whole, w1t.at[slot], lsem.at[slot]).wait()

        def norm(i, _):
            slot = lax.rem(i, 2)

            @pl.when(i + 1 < TOK // RX)
            def _():
                x_copy(i + 1).start()

            x_copy(i).wait()

            def group(j, _):
                r = pl.ds(pl.multiple_of(j * RG, RG), RG)
                o = pl.ds(pl.multiple_of(i * RX + j * RG, RG), RG)
                tiles = [slice(n * 128, (n + 1) * 128) for n in range(D // 128)]
                t = jnp.zeros((RG, 128), F32)
                for n in tiles:
                    t += xs[slot, r, n].astype(F32)
                mu = jnp.sum(t, axis=-1, keepdims=True) * (1.0 / D)
                t = jnp.zeros((RG, 128), F32)
                for n in tiles:
                    d = xs[slot, r, n].astype(F32) - mu
                    t += d * d
                var = jnp.sum(t, axis=-1, keepdims=True) * (1.0 / D)
                rs = lax.rsqrt(var + EPS)
                for n in tiles:
                    d = xs[slot, r, n].astype(F32) - mu
                    xn[o, n] = (d * rs * gamma[:, n]).astype(BF16)
                return 0

            lax.fori_loop(0, RX // RG, group, 0)

            @pl.when(i == 3)
            def _():
                ev_forward(L1, 0)
                ev_direct(L1, 1)
                ev_direct(L1, 2)

            return 0

        lax.fori_loop(0, TOK // RX, norm, 0)
        ev_diag(L1, 0)
        ev_here(L1, 0)
        load_w1(0)

        def run(rows, c0, c1):
            per = TOK // rows

            def out_copies(i):
                slot = lax.rem(i, 2)
                c, m = c0 + lax.div(i, per), lax.rem(i, per)
                r = pl.ds(pl.multiple_of(m * rows, rows), rows)
                return [
                    pltpu.make_async_copy(
                        ht.at[slot, pl.ds(0, rows), pl.ds(half * CH, CH)],
                        h.at[r, half_cols(half, c * CH, CH)],
                        osem.at[slot],
                    )
                    for half in range(2)
                ]

            def wait_out(i):
                slot = lax.rem(i, 2)
                whole = h.at[pl.ds(0, rows), pl.ds(0, 2 * CH)]
                done = ht.at[slot, pl.ds(0, rows)]
                pltpu.make_async_copy(done, whole, osem.at[slot]).wait()

            def step(i, _):
                c, m = c0 + lax.div(i, per), lax.rem(i, per)
                slot = lax.rem(i, 2)
                lead = lax.div(c, EXTRA)
                more = lax.rem(c, EXTRA) == EXTRA - 1
                k = c + 1 + lead
                g = c + 1 + jnp.maximum(lead - 1, 0)

                @pl.when(m == 0)
                def _():
                    wait_w1(c)
                    if c0 > 0:
                        either(ev_diag, g)
                    either(ev_forward, k)
                    if c0 == 0:
                        either(ev_direct, k + 2)
                    else:

                        @pl.when(c == c0)
                        def _():
                            either(ev_direct, k + 2)

                        either(ev_direct, k + 3)

                @pl.when((m == 1) & more)
                def _():
                    either(ev_forward, k + 1)
                    either(ev_direct, k + (3 if c0 == 0 else 4))
                    if c0 > 0:
                        either(ev_diag, g + 1)

                if c0 == 0:

                    @pl.when(m == 2)
                    def _():
                        either(ev_diag, g)

                @pl.when((m == per - 1) & (c + 1 < N1))
                def _():
                    ev_here(L1, c + 1)
                    load_w1(c + 1)

                @pl.when((m == per - 1) & (c + 1 == N1))
                def _():
                    ev_here(L2, N1)
                    ev_here(L2, N1 + 1)
                    load_w2(0)

                @pl.when(i >= 2)
                def _():
                    wait_out(i)

                w = w1t.at[lax.rem(c, 2)]
                for j in range(rows // S1):
                    r = pl.ds(pl.multiple_of(m * rows + j * S1, S1), S1)
                    t = jnp.dot(xn[r, :], w[...], preferred_element_type=F32)
                    ht[slot, j * S1 : (j + 1) * S1, :] = _gelu(t).astype(BF16)
                start(out_copies(i))
                return 0

            lax.fori_loop(0, per * (c1 - c0), step, 0)
            wait_out(0)
            wait_out(1)

        run(R1 // 2, 0, EXTRA)
        run(R1, EXTRA, N1)

    pl.run_scoped(
        first,
        pltpu.VMEM((TOK, D), BF16),
        pltpu.VMEM((2, RX, D), BF16),
        pltpu.VMEM((2, D, 2 * CH), BF16),
        pltpu.VMEM((2, R1, 2 * CH), BF16),
        pltpu.SemaphoreType.DMA((2,)),
        pltpu.SemaphoreType.DMA((2,)),
        pltpu.SemaphoreType.DMA((2,)),
    )

    k_last = N1 + (N1 - 1) // EXTRA + (1 if N1 % EXTRA == 0 else 0)
    per = TOK // R2

    def rest(acc, ht, hsem, asem):
        def load_h(i):
            slot = lax.rem(i, 2)
            s, m = lax.div(i, per), lax.rem(i, per)
            r = pl.ds(pl.multiple_of(m * R2, R2), R2)
            for half in range(2):
                pltpu.make_async_copy(
                    h.at[r, half_cols(half, s * K2, K2)],
                    ht.at[slot, :, pl.ds(half * K2, K2)],
                    hsem.at[slot],
                ).start()

        def wait_h(i):
            slot = lax.rem(i, 2)
            whole = h.at[pl.ds(0, R2), pl.ds(0, 2 * K2)]
            pltpu.make_async_copy(whole, ht.at[slot], hsem.at[slot]).wait()

        def acc_copy(m):
            r = pl.ds(pl.multiple_of(m * R2, R2), R2)
            return pltpu.make_async_copy(acc.at[r, :], acc_out.at[r, :], asem.at[m])

        load_h(0)

        def step(first_slot, i, _):
            s, m = lax.div(i, per), lax.rem(i, per)
            slot = lax.rem(i, 2)
            k = k_last + 1 + 2 * s

            for q in range(2):

                @pl.when(m == 2 * q)
                def _(q=q):
                    second(ev_forward, k + q)
                    second(ev_direct, k + q + 3)

                @pl.when(m == 2 * q + 1)
                def _(q=q):
                    second(ev_diag, k - 1 + q)

            @pl.when(m == 0)
            def _():
                wait_w2(s)

            @pl.when((m == per - 1) & (s + 1 < NS))
            def _():
                ev_here(L2, N1 + 2 * s + 2)
                ev_here(L2, N1 + 2 * s + 3)
                load_w2(s + 1)

            @pl.when(i + 1 < per * NS)
            def _():
                load_h(i + 1)

            wait_h(i)
            w = w2t.at[lax.rem(s, 2)]
            for j in range(R2 // S2):
                r = pl.ds(pl.multiple_of(m * R2 + j * S2, S2), S2)
                for n in range(D // C2):
                    cols = slice(n * C2, (n + 1) * C2)
                    hj = ht[slot, j * S2 : (j + 1) * S2, :]
                    t = jnp.dot(hj, w[:, cols], preferred_element_type=F32)
                    if first_slot:
                        acc[r, cols] = t
                    else:
                        acc[r, cols] += t

            @pl.when(s == NS - 1)
            def _():
                acc_copy(m).start()

            return 0

        lax.fori_loop(0, per, functools.partial(step, True), 0)
        lax.fori_loop(per, per * NS, functools.partial(step, False), 0)
        for m in range(per):
            acc_copy(m).wait()

    pl.run_scoped(
        rest,
        pltpu.VMEM((TOK, D), F32),
        pltpu.VMEM((2, R2, 2 * K2), BF16),
        pltpu.SemaphoreType.DMA((2,)),
        pltpu.SemaphoreType.DMA((per,)),
    )

    ev_diag(L2, NK - 1)

    def last(k, _):
        ev_here(L2, k)
        return 0

    lax.fori_loop(N1 + 2 * NS, NK, last, 0)

    def drain(ln, k, _):
        for c in ln.direct(k) + ln.forward(k) + ln.core_own(k) + ln.core_xy(k) + ln.core_diag(k):
            c.wait_send()
        return 0

    lax.fori_loop(0, N1, functools.partial(drain, L1), 0)
    lax.fori_loop(N1, NK, functools.partial(drain, L2), 0)


def _tail(x, acc, h0, h1, w2, g2, y, wt, sem):
    @pl.when(pl.program_id(0) == 0)
    def _():
        a, b = lax.axis_index("fsdp"), lax.axis_index("tp")
        ax = a + 1 - 2 * lax.rem(a, 2)
        ay = a + 2 - 4 * lax.div(a, 2)
        chips = (a, ax, ay, 3 - a)
        for half in range(2):
            for r in range(4):
                v = (pl.ds(FH - KT, KT), slice(None))
                src = w2.at[v] if half == 0 and r == 0 else g2.at[(half, r, *v)]
                rows = pl.ds(pl.multiple_of((b if half == 0 else 1 - b) * KT, KT), KT)
                cols = pl.ds(pl.multiple_of(chips[r] * DS, 128), DS)
                pltpu.make_async_copy(src, wt.at[rows, cols], sem).start()
        pltpu.make_async_copy(wt, wt, sem).wait()

    for n in range(D // C2):
        cols = slice(n * C2, (n + 1) * C2)
        t = jnp.dot(h0[...], wt[:KT, cols], preferred_element_type=F32)
        t += jnp.dot(h1[...], wt[KT:, cols], preferred_element_type=F32)
        y[:, cols] = (x[:, cols].astype(F32) + (acc[:, cols] + t)).astype(BF16)


def solution(mesh):
    any_ = pl.BlockSpec(memory_space=pl.ANY)

    def body(x, gamma, w1, w2):
        acc, h, _, g2 = pl.pallas_call(
            _kernel,
            out_shape=(
                jax.ShapeDtypeStruct((TOK, D), F32),
                jax.ShapeDtypeStruct((TOK, F), BF16),
                jax.ShapeDtypeStruct((2, 4, DS, FH), BF16),
                jax.ShapeDtypeStruct((2, 4, FH, DS), BF16),
            ),
            in_specs=[any_, pl.BlockSpec(memory_space=pltpu.VMEM), any_, any_],
            out_specs=(any_,) * 4,
            scratch_shapes=[
                pltpu.VMEM((2, 2 * K2, D), BF16),
                pltpu.SemaphoreType.DMA((2, 8, NK)),
                pltpu.SemaphoreType.DMA((2,)),
            ],
            compiler_params=pltpu.CompilerParams(
                collective_id=0, has_side_effects=True, vmem_limit_bytes=67043328
            ),
            name="mlp",
        )(x, gamma.reshape(1, D), w1, w2)
        return pl.pallas_call(
            _tail,
            grid=(TOK // RT,),
            out_shape=jax.ShapeDtypeStruct((TOK, D), BF16),
            in_specs=[
                pl.BlockSpec((RT, D), lambda m: (m, 0)),
                pl.BlockSpec((RT, D), lambda m: (m, 0)),
                pl.BlockSpec((RT, KT), lambda m: (m, FH // KT - 1)),
                pl.BlockSpec((RT, KT), lambda m: (m, F // KT - 1)),
                any_,
                any_,
            ],
            out_specs=pl.BlockSpec((RT, D), lambda m: (m, 0)),
            scratch_shapes=[pltpu.VMEM((2 * KT, D), BF16), pltpu.SemaphoreType.DMA],
            compiler_params=pltpu.CompilerParams(vmem_limit_bytes=60 * 2**20),
            name="tail",
        )(x, acc, h, h, w2, g2)

    return jax.shard_map(
        body,
        mesh=mesh,
        in_specs=(P(("fsdp", "tp"), None), P(None), P("fsdp", "tp"), P("tp", "fsdp")),
        out_specs=P(("fsdp", "tp"), None),
        check_vma=False,
    )
```

```python
import functools

import jax
import jax.numpy as jnp
from jax import lax
from jax.experimental import pallas as pl
from jax.experimental.pallas import tpu as pltpu
from jax.sharding import PartitionSpec as P

EPS = 1e-6
MESH = pl.DeviceIdType.MESH
BF16 = jnp.bfloat16
F32 = jnp.float32

TOK = 4096
D = 2560
F = 10240
FH = F // 2
DS = D // 4
CH = 256
N1 = FH // CH
NK = 2 * N1
R1 = 2048
S1 = 256
R2 = 1024
S2 = 512
RX = 512
RG = 128
C2 = 512
K2 = 2 * CH
NS = FH // K2 - 2
RT = 512
KT = FH - NS * K2
EXTRA = 6

C0 = 0.7978845608028654
C1 = C0 * 0.044715


def _gelu(x):
    hx = 0.5 * x
    return hx + hx * jnp.tanh(x * (C0 + C1 * (x * x)))


def _kernel(x, gamma, w1, w2, acc_out, h, g1, g2, w1t, w2t, ht, sems, wsem):
    a, b = lax.axis_index("fsdp"), lax.axis_index("tp")
    ax = a + 1 - 2 * lax.rem(a, 2)
    ay = a + 2 - 4 * lax.div(a, 2)
    ad = 3 - a
    chips = (a, ax, ay, ad)
    to_x, to_y, to_c = (ax, b), (ay, b), (a, 1 - b)

    def rows1(k, half):
        cols = pl.ds(pl.multiple_of(k * CH, CH), CH)
        if half is None:
            return (slice(None), cols)
        return (pl.ds(half * (DS // 2), DS // 2), cols)

    def rows2(k, half):
        if half is None:
            return (pl.ds(pl.multiple_of((k - N1) * CH, CH), CH), slice(None))
        hc = CH // 2
        return (pl.ds(pl.multiple_of((k - N1) * CH + half * hc, hc), hc), slice(None))

    class Links:
        def __init__(self, w, g, view):
            self.w, self.g, self.view = w, g, view

        def copy(self, kind, k, src, dst, half, dev):
            v = self.view(k, half)
            s = self.w.at[v] if src is None else self.g.at[(*src, *v)]
            return pltpu.make_async_remote_copy(
                src_ref=s,
                dst_ref=self.g.at[(*dst, *v)],
                send_sem=sems.at[0, kind, k],
                recv_sem=sems.at[1, kind, k],
                device_id=dev,
                device_id_type=MESH,
            )

        def direct(self, k):
            return [
                self.copy(0, k, None, (0, 1), None, to_x),
                self.copy(1, k, None, (0, 2), None, to_y),
            ]

        def forward(self, k):
            return [
                self.copy(2, k, (0, 2), (0, 3), 1, to_x),
                self.copy(3, k, (0, 1), (0, 3), 0, to_y),
            ]

        def core_own(self, k):
            return [self.copy(4, k, None, (1, 0), None, to_c)]

        def core_xy(self, k):
            return [
                self.copy(5, k, (0, 1), (1, 1), None, to_c),
                self.copy(6, k, (0, 2), (1, 2), None, to_c),
            ]

        def core_diag(self, k):
            return [self.copy(7, k, (0, 3), (1, 3), None, to_c)]

    L1, L2 = Links(w1, g1, rows1), Links(w2, g2, rows2)

    def start(copies):
        for c in copies:
            c.start()

    def arrived(copies):
        for c in copies:
            c.wait_recv()

    def ev_direct(ln, k):
        start(ln.direct(k))
        start(ln.core_own(k))

    def ev_forward(ln, k):
        arrived(ln.direct(k))
        start(ln.forward(k))
        start(ln.core_xy(k))

    def ev_diag(ln, k):
        arrived(ln.forward(k))
        start(ln.core_diag(k))

    def ev_here(ln, k):
        arrived(ln.core_own(k) + ln.core_xy(k) + ln.core_diag(k))

    def either(ev, k):
        @pl.when(k < N1)
        def _():
            ev(L1, k)

        @pl.when((k >= N1) & (k < NK))
        def _():
            ev(L2, k)

    def second(ev, k):
        @pl.when(k < NK)
        def _():
            ev(L2, k)

    def half_cols(half, start_col, n):
        off = (b if half == 0 else 1 - b) * FH + start_col
        return pl.ds(pl.multiple_of(off, n), n)

    def load_w2(s):
        slot = lax.rem(s, 2)
        v = (pl.ds(pl.multiple_of(s * K2, K2), K2), slice(None))
        for half in range(2):
            for r in range(4):
                src = w2.at[v] if half == 0 and r == 0 else g2.at[(half, r, *v)]
                cols = pl.ds(pl.multiple_of(chips[r] * DS, 128), DS)
                dst = w2t.at[slot, pl.ds(half * K2, K2), cols]
                pltpu.make_async_copy(src, dst, wsem.at[slot]).start()

    def wait_w2(s):
        slot = lax.rem(s, 2)
        whole = h.at[pl.ds(0, 2 * K2), pl.ds(0, D)]
        pltpu.make_async_copy(whole, w2t.at[slot], wsem.at[slot]).wait()

    barrier = pltpu.get_barrier_semaphore()
    for dev in (to_x, to_y, to_c):
        pl.semaphore_signal(barrier, inc=1, device_id=dev, device_id_type=MESH)
    pl.semaphore_wait(barrier, 3)
    ev_direct(L1, 0)

    def first(xn, xs, xsem, lsem, osem):
        def x_copy(i):
            slot = lax.rem(i, 2)
            r = pl.ds(pl.multiple_of(i * RX, RX), RX)
            return pltpu.make_async_copy(x.at[r, :], xs.at[slot], xsem.at[slot])

        x_copy(0).start()

        def load_w1(c):
            slot = lax.rem(c, 2)
            v = rows1(c, None)
            for half in range(2):
                for r in range(4):
                    src = w1.at[v] if half == 0 and r == 0 else g1.at[(half, r, *v)]
                    rows = pl.ds(pl.multiple_of(chips[r] * DS, 128), DS)
                    dst = w1t.at[slot, rows, pl.ds(half * CH, CH)]
                    pltpu.make_async_copy(src, dst, lsem.at[slot]).start()

        def wait_w1(c):
            slot = lax.rem(c, 2)
            whole = h.at[pl.ds(0, D), pl.ds(0, 2 * CH)]
            pltpu.make_async_copy(whole, w1t.at[slot], lsem.at[slot]).wait()

        def norm(i, _):
            slot = lax.rem(i, 2)

            @pl.when(i + 1 < TOK // RX)
            def _():
                x_copy(i + 1).start()

            x_copy(i).wait()

            def group(j, _):
                r = pl.ds(pl.multiple_of(j * RG, RG), RG)
                o = pl.ds(pl.multiple_of(i * RX + j * RG, RG), RG)
                tiles = [slice(n * 128, (n + 1) * 128) for n in range(D // 128)]
                t = jnp.zeros((RG, 128), F32)
                for n in tiles:
                    t += xs[slot, r, n].astype(F32)
                mu = jnp.sum(t, axis=-1, keepdims=True) * (1.0 / D)
                t = jnp.zeros((RG, 128), F32)
                for n in tiles:
                    d = xs[slot, r, n].astype(F32) - mu
                    t += d * d
                var = jnp.sum(t, axis=-1, keepdims=True) * (1.0 / D)
                rs = lax.rsqrt(var + EPS)
                for n in tiles:
                    d = xs[slot, r, n].astype(F32) - mu
                    xn[o, n] = (d * rs * gamma[:, n]).astype(BF16)
                return 0

            lax.fori_loop(0, RX // RG, group, 0)

            @pl.when(i == 3)
            def _():
                ev_forward(L1, 0)
                ev_direct(L1, 1)
                ev_direct(L1, 2)

            return 0

        lax.fori_loop(0, TOK // RX, norm, 0)
        ev_diag(L1, 0)
        ev_here(L1, 0)
        load_w1(0)

        def run(rows, c0, c1):
            per = TOK // rows

            def out_copies(i):
                slot = lax.rem(i, 2)
                c, m = c0 + lax.div(i, per), lax.rem(i, per)
                return [
                    pltpu.make_async_copy(
                        ht.at[slot, :, pl.ds(p * 2 * CH + half * CH, CH)],
                        h.at[
                            pl.ds(pl.multiple_of(m * rows + p * R2, R2), R2),
                            half_cols(half, c * CH, CH),
                        ],
                        osem.at[slot],
                    )
                    for p in range(rows // R2)
                    for half in range(2)
                ]

            def wait_out(i):
                slot = lax.rem(i, 2)
                cols = pl.ds(0, (rows // R2) * 2 * CH)
                done = ht.at[slot, :, cols]
                pltpu.make_async_copy(done, h.at[pl.ds(0, R2), cols], osem.at[slot]).wait()

            def step(i, _):
                c, m = c0 + lax.div(i, per), lax.rem(i, per)
                slot = lax.rem(i, 2)
                lead = lax.div(c, EXTRA)
                more = lax.rem(c, EXTRA) == EXTRA - 1
                k = c + 1 + lead
                g = c + 1 + jnp.maximum(lead - 1, 0)

                @pl.when(m == 0)
                def _():
                    wait_w1(c)
                    if c0 > 0:
                        either(ev_diag, g)
                    either(ev_forward, k)
                    if c0 == 0:
                        either(ev_direct, k + 2)
                    else:

                        @pl.when(c == c0)
                        def _():
                            either(ev_direct, k + 2)

                        either(ev_direct, k + 3)

                @pl.when((m == 1) & more)
                def _():
                    either(ev_forward, k + 1)
                    either(ev_direct, k + (3 if c0 == 0 else 4))
                    if c0 > 0:
                        either(ev_diag, g + 1)

                if c0 == 0:

                    @pl.when(m == 2)
                    def _():
                        either(ev_diag, g)

                @pl.when((m == per - 1) & (c + 1 < N1))
                def _():
                    ev_here(L1, c + 1)
                    load_w1(c + 1)

                @pl.when((m == per - 1) & (c + 1 == N1))
                def _():
                    ev_here(L2, N1)
                    ev_here(L2, N1 + 1)
                    load_w2(0)

                @pl.when(i >= 2)
                def _():
                    wait_out(i)

                w = w1t.at[lax.rem(c, 2)]
                for j in range(rows // S1):
                    r = pl.ds(pl.multiple_of(m * rows + j * S1, S1), S1)
                    t = jnp.dot(xn[r, :], w[...], preferred_element_type=F32)
                    p, q = divmod(j * S1, R2)
                    cols = slice(p * 2 * CH, (p + 1) * 2 * CH)
                    ht[slot, q : q + S1, cols] = _gelu(t).astype(BF16)
                start(out_copies(i))
                return 0

            lax.fori_loop(0, per * (c1 - c0), step, 0)
            wait_out(0)
            wait_out(1)

        run(R1 // 2, 0, EXTRA)
        run(R1, EXTRA, N1)

    pl.run_scoped(
        first,
        pltpu.VMEM((TOK, D), BF16),
        pltpu.VMEM((2, RX, D), BF16),
        pltpu.SemaphoreType.DMA((2,)),
        pltpu.SemaphoreType.DMA((2,)),
        pltpu.SemaphoreType.DMA((2,)),
    )

    k_last = N1 + (N1 - 1) // EXTRA + (1 if N1 % EXTRA == 0 else 0)
    per = TOK // R2

    def rest(acc, hsem, asem):
        def load_h(i):
            slot = lax.rem(i, 2)
            s, m = lax.div(i, per), lax.rem(i, per)
            r = pl.ds(pl.multiple_of(m * R2, R2), R2)
            for half in range(2):
                pltpu.make_async_copy(
                    h.at[r, half_cols(half, s * K2, K2)],
                    ht.at[slot, :, pl.ds(half * K2, K2)],
                    hsem.at[slot],
                ).start()

        def wait_h(i):
            slot = lax.rem(i, 2)
            whole = h.at[pl.ds(0, R2), pl.ds(0, 2 * K2)]
            pltpu.make_async_copy(whole, ht.at[slot], hsem.at[slot]).wait()

        def acc_copy(m):
            r = pl.ds(pl.multiple_of(m * R2, R2), R2)
            return pltpu.make_async_copy(acc.at[r, :], acc_out.at[r, :], asem.at[m])

        load_h(0)

        def step(first_slot, i, _):
            s, m = lax.div(i, per), lax.rem(i, per)
            slot = lax.rem(i, 2)
            k = k_last + 1 + 2 * s

            for q in range(2):

                @pl.when(m == 2 * q)
                def _(q=q):
                    second(ev_forward, k + q)
                    second(ev_direct, k + q + 3)

                @pl.when(m == 2 * q + 1)
                def _(q=q):
                    second(ev_diag, k - 1 + q)

            @pl.when(m == 0)
            def _():
                wait_w2(s)

            @pl.when((m == per - 1) & (s + 1 < NS))
            def _():
                ev_here(L2, N1 + 2 * s + 2)
                ev_here(L2, N1 + 2 * s + 3)
                load_w2(s + 1)

            @pl.when(i + 1 < per * NS)
            def _():
                load_h(i + 1)

            wait_h(i)
            w = w2t.at[lax.rem(s, 2)]
            for j in range(R2 // S2):
                r = pl.ds(pl.multiple_of(m * R2 + j * S2, S2), S2)
                for n in range(D // C2):
                    cols = slice(n * C2, (n + 1) * C2)
                    hj = ht[slot, j * S2 : (j + 1) * S2, :]
                    t = jnp.dot(hj, w[:, cols], preferred_element_type=F32)
                    if first_slot:
                        acc[r, cols] = t
                    else:
                        acc[r, cols] += t

            @pl.when(s == NS - 1)
            def _():
                acc_copy(m).start()

            return 0

        lax.fori_loop(0, per, functools.partial(step, True), 0)
        lax.fori_loop(per, per * NS, functools.partial(step, False), 0)
        for m in range(per):
            acc_copy(m).wait()

    pl.run_scoped(
        rest,
        pltpu.VMEM((TOK, D), F32),
        pltpu.SemaphoreType.DMA((2,)),
        pltpu.SemaphoreType.DMA((per,)),
    )

    ev_diag(L2, NK - 1)

    def last(k, _):
        ev_here(L2, k)
        return 0

    lax.fori_loop(N1 + 2 * NS, NK, last, 0)

    def drain(ln, k, _):
        for c in ln.direct(k) + ln.forward(k) + ln.core_own(k) + ln.core_xy(k) + ln.core_diag(k):
            c.wait_send()
        return 0

    lax.fori_loop(0, N1, functools.partial(drain, L1), 0)
    lax.fori_loop(N1, NK, functools.partial(drain, L2), 0)


def _tail(x, acc, h0, h1, w2, g2, y, wt, sem):
    @pl.when(pl.program_id(0) == 0)
    def _():
        a, b = lax.axis_index("fsdp"), lax.axis_index("tp")
        ax = a + 1 - 2 * lax.rem(a, 2)
        ay = a + 2 - 4 * lax.div(a, 2)
        chips = (a, ax, ay, 3 - a)
        for half in range(2):
            for r in range(4):
                v = (pl.ds(FH - KT, KT), slice(None))
                src = w2.at[v] if half == 0 and r == 0 else g2.at[(half, r, *v)]
                rows = pl.ds(pl.multiple_of((b if half == 0 else 1 - b) * KT, KT), KT)
                cols = pl.ds(pl.multiple_of(chips[r] * DS, 128), DS)
                pltpu.make_async_copy(src, wt.at[rows, cols], sem).start()
        pltpu.make_async_copy(wt, wt, sem).wait()

    for n in range(D // C2):
        cols = slice(n * C2, (n + 1) * C2)
        t = jnp.dot(h0[...], wt[:KT, cols], preferred_element_type=F32)
        t += jnp.dot(h1[...], wt[KT:, cols], preferred_element_type=F32)
        y[:, cols] = (x[:, cols].astype(F32) + (acc[:, cols] + t)).astype(BF16)


def solution(mesh):
    any_ = pl.BlockSpec(memory_space=pl.ANY)

    def body(x, gamma, w1, w2):
        acc, h, _, g2 = pl.pallas_call(
            _kernel,
            out_shape=(
                jax.ShapeDtypeStruct((TOK, D), F32),
                jax.ShapeDtypeStruct((TOK, F), BF16),
                jax.ShapeDtypeStruct((2, 4, DS, FH), BF16),
                jax.ShapeDtypeStruct((2, 4, FH, DS), BF16),
            ),
            in_specs=[any_, pl.BlockSpec(memory_space=pltpu.VMEM), any_, any_],
            out_specs=(any_,) * 4,
            scratch_shapes=[
                pltpu.VMEM((2, D, 2 * CH), BF16),
                pltpu.VMEM((2, 2 * K2, D), BF16),
                pltpu.VMEM((2, R2, 2 * K2), BF16),
                pltpu.SemaphoreType.DMA((2, 8, NK)),
                pltpu.SemaphoreType.DMA((2,)),
            ],
            compiler_params=pltpu.CompilerParams(
                collective_id=0, has_side_effects=True, vmem_limit_bytes=67043328
            ),
            name="mlp",
        )(x, gamma.reshape(1, D), w1, w2)
        return pl.pallas_call(
            _tail,
            grid=(TOK // RT,),
            out_shape=jax.ShapeDtypeStruct((TOK, D), BF16),
            in_specs=[
                pl.BlockSpec((RT, D), lambda m: (m, 0)),
                pl.BlockSpec((RT, D), lambda m: (m, 0)),
                pl.BlockSpec((RT, KT), lambda m: (m, FH // KT - 1)),
                pl.BlockSpec((RT, KT), lambda m: (m, F // KT - 1)),
                any_,
                any_,
            ],
            out_specs=pl.BlockSpec((RT, D), lambda m: (m, 0)),
            scratch_shapes=[pltpu.VMEM((2 * KT, D), BF16), pltpu.SemaphoreType.DMA],
            compiler_params=pltpu.CompilerParams(vmem_limit_bytes=60 * 2**20),
            name="tail",
        )(x, acc, h, h, w2, g2)

    return jax.shard_map(
        body,
        mesh=mesh,
        in_specs=(P(("fsdp", "tp"), None), P(None), P("fsdp", "tp"), P("tp", "fsdp")),
        out_specs=P(("fsdp", "tp"), None),
        check_vma=False,
    )
```

```python
import functools

import jax
import jax.numpy as jnp
from jax import lax
from jax.experimental import pallas as pl
from jax.experimental.pallas import tpu as pltpu
from jax.sharding import PartitionSpec as P

EPS = 1e-6
MESH = pl.DeviceIdType.MESH
BF16 = jnp.bfloat16
F32 = jnp.float32

TOK = 4096
D = 2560
F = 10240
FH = F // 2
DS = D // 4
CH = 256
N1 = FH // CH
NK = 2 * N1
R1 = 2048
S1 = 256
R2 = 1024
S2 = 512
RX = 512
RG = 128
C2 = 512
K2 = 2 * CH
NS = FH // K2 - 1
RT = 512
KT = FH - NS * K2
EXTRA = 7

C0 = 0.7978845608028654
C1 = C0 * 0.044715


def _gelu(x):
    hx = 0.5 * x
    return hx + hx * jnp.tanh(x * (C0 + C1 * (x * x)))


def _kernel(x, gamma, w1, w2, acc_out, h, g1, g2, w1t, w2t, ht, sems, wsem):
    a, b = lax.axis_index("fsdp"), lax.axis_index("tp")
    ax = a + 1 - 2 * lax.rem(a, 2)
    ay = a + 2 - 4 * lax.div(a, 2)
    ad = 3 - a
    chips = (a, ax, ay, ad)
    to_x, to_y, to_c = (ax, b), (ay, b), (a, 1 - b)

    def rows1(k, half):
        cols = pl.ds(pl.multiple_of(k * CH, CH), CH)
        if half is None:
            return (slice(None), cols)
        return (pl.ds(half * (DS // 2), DS // 2), cols)

    def rows2(k, half):
        if half is None:
            return (pl.ds(pl.multiple_of((k - N1) * CH, CH), CH), slice(None))
        hc = CH // 2
        return (pl.ds(pl.multiple_of((k - N1) * CH + half * hc, hc), hc), slice(None))

    class Links:
        def __init__(self, w, g, view):
            self.w, self.g, self.view = w, g, view

        def copy(self, kind, k, src, dst, half, dev):
            v = self.view(k, half)
            s = self.w.at[v] if src is None else self.g.at[(*src, *v)]
            return pltpu.make_async_remote_copy(
                src_ref=s,
                dst_ref=self.g.at[(*dst, *v)],
                send_sem=sems.at[0, kind, k],
                recv_sem=sems.at[1, kind, k],
                device_id=dev,
                device_id_type=MESH,
            )

        def direct(self, k):
            return [
                self.copy(0, k, None, (0, 1), None, to_x),
                self.copy(1, k, None, (0, 2), None, to_y),
            ]

        def forward(self, k):
            return [
                self.copy(2, k, (0, 2), (0, 3), 1, to_x),
                self.copy(3, k, (0, 1), (0, 3), 0, to_y),
            ]

        def core_own(self, k):
            return [self.copy(4, k, None, (1, 0), None, to_c)]

        def core_xy(self, k):
            return [
                self.copy(5, k, (0, 1), (1, 1), None, to_c),
                self.copy(6, k, (0, 2), (1, 2), None, to_c),
            ]

        def core_diag(self, k):
            return [self.copy(7, k, (0, 3), (1, 3), None, to_c)]

    L1, L2 = Links(w1, g1, rows1), Links(w2, g2, rows2)

    def start(copies):
        for c in copies:
            c.start()

    def arrived(copies):
        for c in copies:
            c.wait_recv()

    def ev_direct(ln, k):
        start(ln.direct(k))
        start(ln.core_own(k))

    def ev_forward(ln, k):
        arrived(ln.direct(k))
        start(ln.forward(k))
        start(ln.core_xy(k))

    def ev_diag(ln, k):
        arrived(ln.forward(k))
        start(ln.core_diag(k))

    def ev_here(ln, k):
        arrived(ln.core_own(k) + ln.core_xy(k) + ln.core_diag(k))

    def either(ev, k):
        @pl.when(k < N1)
        def _():
            ev(L1, k)

        @pl.when((k >= N1) & (k < NK))
        def _():
            ev(L2, k)

    def second(ev, k):
        @pl.when(k < NK)
        def _():
            ev(L2, k)

    def half_cols(half, start_col, n):
        off = (b if half == 0 else 1 - b) * FH + start_col
        return pl.ds(pl.multiple_of(off, n), n)

    def load_w2(s):
        slot = lax.rem(s, 2)
        v = (pl.ds(pl.multiple_of(s * K2, K2), K2), slice(None))
        for half in range(2):
            for r in range(4):
                src = w2.at[v] if half == 0 and r == 0 else g2.at[(half, r, *v)]
                cols = pl.ds(pl.multiple_of(chips[r] * DS, 128), DS)
                dst = w2t.at[slot, pl.ds(half * K2, K2), cols]
                pltpu.make_async_copy(src, dst, wsem.at[slot]).start()

    def wait_w2(s):
        slot = lax.rem(s, 2)
        whole = h.at[pl.ds(0, 2 * K2), pl.ds(0, D)]
        pltpu.make_async_copy(whole, w2t.at[slot], wsem.at[slot]).wait()

    barrier = pltpu.get_barrier_semaphore()
    for dev in (to_x, to_y, to_c):
        pl.semaphore_signal(barrier, inc=1, device_id=dev, device_id_type=MESH)
    pl.semaphore_wait(barrier, 3)
    ev_direct(L1, 0)

    def first(xn, xs, xsem, lsem, osem):
        def x_copy(i):
            slot = lax.rem(i, 2)
            r = pl.ds(pl.multiple_of(i * RX, RX), RX)
            return pltpu.make_async_copy(x.at[r, :], xs.at[slot], xsem.at[slot])

        x_copy(0).start()

        def load_w1(c):
            slot = lax.rem(c, 2)
            v = rows1(c, None)
            for half in range(2):
                for r in range(4):
                    src = w1.at[v] if half == 0 and r == 0 else g1.at[(half, r, *v)]
                    rows = pl.ds(pl.multiple_of(chips[r] * DS, 128), DS)
                    dst = w1t.at[slot, rows, pl.ds(half * CH, CH)]
                    pltpu.make_async_copy(src, dst, lsem.at[slot]).start()

        def wait_w1(c):
            slot = lax.rem(c, 2)
            whole = h.at[pl.ds(0, D), pl.ds(0, 2 * CH)]
            pltpu.make_async_copy(whole, w1t.at[slot], lsem.at[slot]).wait()

        def norm(i, _):
            slot = lax.rem(i, 2)

            @pl.when(i + 1 < TOK // RX)
            def _():
                x_copy(i + 1).start()

            x_copy(i).wait()

            def group(j, _):
                r = pl.ds(pl.multiple_of(j * RG, RG), RG)
                o = pl.ds(pl.multiple_of(i * RX + j * RG, RG), RG)
                tiles = [slice(n * 128, (n + 1) * 128) for n in range(D // 128)]
                t = jnp.zeros((RG, 128), F32)
                for n in tiles:
                    t += xs[slot, r, n].astype(F32)
                mu = jnp.sum(t, axis=-1, keepdims=True) * (1.0 / D)
                t = jnp.zeros((RG, 128), F32)
                for n in tiles:
                    d = xs[slot, r, n].astype(F32) - mu
                    t += d * d
                var = jnp.sum(t, axis=-1, keepdims=True) * (1.0 / D)
                rs = lax.rsqrt(var + EPS)
                for n in tiles:
                    d = xs[slot, r, n].astype(F32) - mu
                    xn[o, n] = (d * rs * gamma[:, n]).astype(BF16)
                return 0

            lax.fori_loop(0, RX // RG, group, 0)

            @pl.when(i == 3)
            def _():
                ev_forward(L1, 0)
                ev_direct(L1, 1)
                ev_direct(L1, 2)

            return 0

        lax.fori_loop(0, TOK // RX, norm, 0)
        ev_diag(L1, 0)
        ev_here(L1, 0)
        load_w1(0)

        def run(rows, c0, c1):
            per = TOK // rows

            def out_copies(i):
                slot = lax.rem(i, 2)
                c, m = c0 + lax.div(i, per), lax.rem(i, per)
                return [
                    pltpu.make_async_copy(
                        ht.at[slot, :, pl.ds(p * 2 * CH + half * CH, CH)],
                        h.at[
                            pl.ds(pl.multiple_of(m * rows + p * R2, R2), R2),
                            half_cols(half, c * CH, CH),
                        ],
                        osem.at[slot],
                    )
                    for p in range(rows // R2)
                    for half in range(2)
                ]

            def wait_out(i):
                slot = lax.rem(i, 2)
                cols = pl.ds(0, (rows // R2) * 2 * CH)
                done = ht.at[slot, :, cols]
                pltpu.make_async_copy(done, h.at[pl.ds(0, R2), cols], osem.at[slot]).wait()

            def step(i, _):
                c, m = c0 + lax.div(i, per), lax.rem(i, per)
                slot = lax.rem(i, 2)
                lead = lax.div(c, EXTRA)
                more = lax.rem(c, EXTRA) == EXTRA - 1
                k = c + 1 + lead
                g = c + 1 + jnp.maximum(lead - 1, 0)

                @pl.when(m == 0)
                def _():
                    wait_w1(c)
                    if c0 > 0:
                        either(ev_diag, g)
                    either(ev_forward, k)
                    if c0 == 0:
                        either(ev_direct, k + 2)
                    else:

                        @pl.when(c == c0)
                        def _():
                            either(ev_direct, k + 2)

                        either(ev_direct, k + 3)

                @pl.when((m == 1) & more)
                def _():
                    either(ev_forward, k + 1)
                    either(ev_direct, k + (3 if c0 == 0 else 4))
                    if c0 > 0:
                        either(ev_diag, g + 1)

                if c0 == 0:

                    @pl.when(m == 2)
                    def _():
                        either(ev_diag, g)

                @pl.when((m == per - 1) & (c + 1 < N1))
                def _():
                    ev_here(L1, c + 1)
                    load_w1(c + 1)

                @pl.when((m == per - 1) & (c + 1 == N1))
                def _():
                    ev_here(L2, N1)
                    ev_here(L2, N1 + 1)
                    load_w2(0)

                @pl.when(i >= 2)
                def _():
                    wait_out(i)

                w = w1t.at[lax.rem(c, 2)]
                for j in range(rows // S1):
                    r = pl.ds(pl.multiple_of(m * rows + j * S1, S1), S1)
                    t = jnp.dot(xn[r, :], w[...], preferred_element_type=F32)
                    p, q = divmod(j * S1, R2)
                    cols = slice(p * 2 * CH, (p + 1) * 2 * CH)
                    ht[slot, q : q + S1, cols] = _gelu(t).astype(BF16)
                start(out_copies(i))
                return 0

            lax.fori_loop(0, per * (c1 - c0), step, 0)
            wait_out(0)
            wait_out(1)

        run(R1 // 2, 0, EXTRA)
        run(R1, EXTRA, N1)

    pl.run_scoped(
        first,
        pltpu.VMEM((TOK, D), BF16),
        pltpu.VMEM((2, RX, D), BF16),
        pltpu.SemaphoreType.DMA((2,)),
        pltpu.SemaphoreType.DMA((2,)),
        pltpu.SemaphoreType.DMA((2,)),
    )

    k_last = N1 + (N1 - 1) // EXTRA + (1 if N1 % EXTRA == 0 else 0)
    per = TOK // R2

    def rest(acc, hsem, asem):
        def load_h(i):
            slot = lax.rem(i, 2)
            s, m = lax.div(i, per), lax.rem(i, per)
            r = pl.ds(pl.multiple_of(m * R2, R2), R2)
            for half in range(2):
                pltpu.make_async_copy(
                    h.at[r, half_cols(half, s * K2, K2)],
                    ht.at[slot, :, pl.ds(half * K2, K2)],
                    hsem.at[slot],
                ).start()

        def wait_h(i):
            slot = lax.rem(i, 2)
            whole = h.at[pl.ds(0, R2), pl.ds(0, 2 * K2)]
            pltpu.make_async_copy(whole, ht.at[slot], hsem.at[slot]).wait()

        def acc_copy(m):
            r = pl.ds(pl.multiple_of(m * R2, R2), R2)
            return pltpu.make_async_copy(acc.at[r, :], acc_out.at[r, :], asem.at[m])

        load_h(0)

        def step(first_slot, i, _):
            s, m = lax.div(i, per), lax.rem(i, per)
            slot = lax.rem(i, 2)
            k = k_last + 1 + 2 * s

            @pl.when(m == 0)
            def _():
                second(ev_diag, k - 1)
                second(ev_forward, k)
                second(ev_direct, k + 3)

            @pl.when(m == 1)
            def _():
                second(ev_diag, k)

            @pl.when(m == 2)
            def _():
                second(ev_forward, k + 1)
                second(ev_direct, k + 4)

            @pl.when(m == 0)
            def _():
                wait_w2(s)

            @pl.when((m == per - 1) & (s + 1 < NS))
            def _():
                ev_here(L2, N1 + 2 * s + 2)
                ev_here(L2, N1 + 2 * s + 3)
                load_w2(s + 1)

            @pl.when(i + 1 < per * NS)
            def _():
                load_h(i + 1)

            wait_h(i)
            w = w2t.at[lax.rem(s, 2)]
            for j in range(R2 // S2):
                r = pl.ds(pl.multiple_of(m * R2 + j * S2, S2), S2)
                for n in range(D // C2):
                    cols = slice(n * C2, (n + 1) * C2)
                    hj = ht[slot, j * S2 : (j + 1) * S2, :]
                    t = jnp.dot(hj, w[:, cols], preferred_element_type=F32)
                    if first_slot:
                        acc[r, cols] = t
                    else:
                        acc[r, cols] += t

            @pl.when(s == NS - 1)
            def _():
                acc_copy(m).start()

            return 0

        lax.fori_loop(0, per, functools.partial(step, True), 0)
        lax.fori_loop(per, per * NS, functools.partial(step, False), 0)
        for m in range(per):
            acc_copy(m).wait()

    pl.run_scoped(
        rest,
        pltpu.VMEM((TOK, D), F32),
        pltpu.SemaphoreType.DMA((2,)),
        pltpu.SemaphoreType.DMA((per,)),
    )

    def last(k, _):
        ev_here(L2, k)
        return 0

    lax.fori_loop(N1 + 2 * NS, NK, last, 0)

    def drain(ln, k, _):
        for c in ln.direct(k) + ln.forward(k) + ln.core_own(k) + ln.core_xy(k) + ln.core_diag(k):
            c.wait_send()
        return 0

    lax.fori_loop(0, N1, functools.partial(drain, L1), 0)
    lax.fori_loop(N1, NK, functools.partial(drain, L2), 0)


def _tail(x, acc, h0, h1, w2, g2, y, wt, sem):
    @pl.when(pl.program_id(0) == 0)
    def _():
        a, b = lax.axis_index("fsdp"), lax.axis_index("tp")
        ax = a + 1 - 2 * lax.rem(a, 2)
        ay = a + 2 - 4 * lax.div(a, 2)
        chips = (a, ax, ay, 3 - a)
        for half in range(2):
            for r in range(4):
                v = (pl.ds(FH - KT, KT), slice(None))
                src = w2.at[v] if half == 0 and r == 0 else g2.at[(half, r, *v)]
                rows = pl.ds(pl.multiple_of((b if half == 0 else 1 - b) * KT, KT), KT)
                cols = pl.ds(pl.multiple_of(chips[r] * DS, 128), DS)
                pltpu.make_async_copy(src, wt.at[rows, cols], sem).start()
        pltpu.make_async_copy(wt, wt, sem).wait()

    for n in range(D // C2):
        cols = slice(n * C2, (n + 1) * C2)
        t = jnp.dot(h0[...], wt[:KT, cols], preferred_element_type=F32)
        t += jnp.dot(h1[...], wt[KT:, cols], preferred_element_type=F32)
        y[:, cols] = (x[:, cols].astype(F32) + (acc[:, cols] + t)).astype(BF16)


def solution(mesh):
    any_ = pl.BlockSpec(memory_space=pl.ANY)

    def body(x, gamma, w1, w2):
        acc, h, _, g2 = pl.pallas_call(
            _kernel,
            out_shape=(
                jax.ShapeDtypeStruct((TOK, D), F32),
                jax.ShapeDtypeStruct((TOK, F), BF16),
                jax.ShapeDtypeStruct((2, 4, DS, FH), BF16),
                jax.ShapeDtypeStruct((2, 4, FH, DS), BF16),
            ),
            in_specs=[any_, pl.BlockSpec(memory_space=pltpu.VMEM), any_, any_],
            out_specs=(any_,) * 4,
            scratch_shapes=[
                pltpu.VMEM((2, D, 2 * CH), BF16),
                pltpu.VMEM((2, 2 * K2, D), BF16),
                pltpu.VMEM((2, R2, 2 * K2), BF16),
                pltpu.SemaphoreType.DMA((2, 8, NK)),
                pltpu.SemaphoreType.DMA((2,)),
            ],
            compiler_params=pltpu.CompilerParams(
                collective_id=0, has_side_effects=True, vmem_limit_bytes=67043328
            ),
            name="mlp",
        )(x, gamma.reshape(1, D), w1, w2)
        return pl.pallas_call(
            _tail,
            grid=(TOK // RT,),
            out_shape=jax.ShapeDtypeStruct((TOK, D), BF16),
            in_specs=[
                pl.BlockSpec((RT, D), lambda m: (m, 0)),
                pl.BlockSpec((RT, D), lambda m: (m, 0)),
                pl.BlockSpec((RT, KT), lambda m: (m, FH // KT - 1)),
                pl.BlockSpec((RT, KT), lambda m: (m, F // KT - 1)),
                any_,
                any_,
            ],
            out_specs=pl.BlockSpec((RT, D), lambda m: (m, 0)),
            scratch_shapes=[pltpu.VMEM((2 * KT, D), BF16), pltpu.SemaphoreType.DMA],
            compiler_params=pltpu.CompilerParams(vmem_limit_bytes=60 * 2**20),
            name="tail",
        )(x, acc, h, h, w2, g2)

    return jax.shard_map(
        body,
        mesh=mesh,
        in_specs=(P(("fsdp", "tp"), None), P(None), P("fsdp", "tp"), P("tp", "fsdp")),
        out_specs=P(("fsdp", "tp"), None),
        check_vma=False,
    )
```
